512 devices in a mesh: seq: 64 (over x, z, core), tensor: 8 (over y).
Axes of the slice: x: 4, y: 8, z: 8, core: 2. Of those that a mesh axis runs over, the one named last changes fastest.
Arguments:
- layer_input: bfloat16 [16384, 2048], P('seq', 'tensor'), may hold values from -4 to 4
- queries: bfloat16 [16384, 4096], P('seq', 'tensor'), may hold values from -160 to 160
- key_values: bfloat16 [2, 16384, 1024], P(None, 'seq', 'tensor'), may hold values from -4.5 to 4.5
- attention_out: bfloat16 [16384, 4096], P('seq', 'tensor'), may hold values from -6 to 6
- output_grad: bfloat16 [16384, 4096], P('seq', 'tensor'), may hold values from -24 to 24
- document_start: int32 [16384], P('seq'), may hold values from 0 to 16383, as said below
Outputs:
- query_grad: bfloat16 [16384, 4096], P('seq', 'tensor')
- key_value_grad: bfloat16 [2, 16384, 1024], P(None, 'seq', 'tensor')
- query_weight_grad: float32 [2048, 4096], P('seq', 'tensor')
The draws below stay inside these ranges and needn't reach their ends.
Inputs may be any that keep to these rules, and one draw needn't show every extreme that they name: Non-decreasing; entry i is the position of the first token of token i's document, so i - 512 < document_start[i] <= i and document_start[document_start[i]] = document_start[i]; some token lies exactly 511 positions after its document's first token.
All inputs are finite; a program needn't handle non-finite values.
Results may differ from the reference program's by a relative error of at most 0.008.
Values may be sent and summed in bfloat16 or wider, within the bound.
No kernel may reach another device: no remote copies, remote signals or barrier semaphores. Data moves between devices by JAX's collectives and lax.ppermute only.
A program may use at most 64 MiB of HBM per device.

```python
import math
import jax
import jax.numpy as jnp
from jax import lax

HEADS = 32
KV_HEADS = 8
HD = 128
D_IN = 2048
TOK_DEV = 256
REACH = 2
MOST = 512
TOKENS = 16384


def document_layout(key):
    lengths = jax.random.randint(jax.random.fold_in(key, 11), (TOKENS,), MOST // 4, MOST + 1)
    chosen = jax.random.randint(jax.random.fold_in(key, 12), (), 0, 4)
    position = jnp.arange(TOKENS, dtype=jnp.int32)
    lengths = jnp.where(position == chosen, MOST, lengths).astype(jnp.int32)
    finish = jnp.cumsum(lengths)
    begins = finish - lengths
    marks = jnp.zeros((TOKENS,), jnp.int32).at[begins].set(1, mode='drop')
    return lax.cummax(jnp.where(marks > 0, position, 0), axis=0).astype(jnp.int32)


def attention_pair(key):
    key_rows = jnp.clip(jax.random.normal(jax.random.fold_in(key, 21), (TOKENS, KV_HEADS, HD), jnp.float32), -4.5, 4.5)
    value_rows = jnp.clip(jax.random.normal(jax.random.fold_in(key, 22), (TOKENS, KV_HEADS, HD), jnp.float32), -4.5, 4.5)
    query_rows = jnp.clip(jax.random.normal(jax.random.fold_in(key, 23), (TOKENS, HEADS, HD), jnp.float32), -4.5, 4.5)
    pairs = jnp.stack((key_rows.reshape(TOKENS, KV_HEADS * HD), value_rows.reshape(TOKENS, KV_HEADS * HD)))
    return (query_rows.reshape(TOKENS, HEADS * HD), pairs)


def draw_document_start(key, part):
    return document_layout(key)


def draw_queries(key, part):
    return attention_pair(key)[0].astype(jnp.bfloat16)


def draw_key_values(key, part):
    return attention_pair(key)[1].astype(jnp.bfloat16)


def with_spikes(result, key, source, target, parts, factor):
    def block_of(dim):
        return (jnp.arange(result.shape[dim]) // (result.shape[dim] // parts)).reshape((-1,) + (1,) * (result.ndim - 1 - dim))

    near = jax.random.permutation(key, parts)[block_of(target)]
    second = (block_of(target) + parts // 2) % parts
    return jnp.where((block_of(source) == near) | (block_of(source) == second), factor * result, result)


def levels(stream_key, dims, pieces, low, largest):
    def one(axis_at, blocks):
        draws = jax.random.uniform(jax.random.fold_in(jax.random.fold_in(stream_key, 6), axis_at), (blocks,), jnp.float32, low / len(pieces), largest / len(pieces))
        return jnp.repeat(jnp.exp(draws), dims[axis_at] // blocks).reshape((-1,) + (1,) * (len(dims) - axis_at - 1))

    level = one(*pieces[0])
    for cut in pieces[1:]:
        level = level * one(*cut)
    return level


def centred(stream_key, shape, scale, most, shards=(), kind=jnp.bfloat16):
    values = scale * jax.random.normal(stream_key, shape, jnp.float32)
    if shards:
        values = values * levels(stream_key, shape, shards, -0.22, 0.18)
    return jnp.clip(values, -most, most).astype(kind)


def noise_with(stream_key, extent, width, bound, pieces, heavy, kind=jnp.bfloat16):
    entries = width * jax.random.normal(stream_key, extent, jnp.float32)
    if pieces:
        entries = entries * levels(stream_key, extent, pieces, -0.22, 0.18)
    return jnp.clip(with_spikes(entries, jax.random.fold_in(stream_key, 3), *heavy), -bound, bound).astype(kind)


def setup_inputs(seed: int = 0) -> dict:
    seeds = jax.random.split(jax.random.key(seed), 7)
    return {
        "layer_input": noise_with(seeds[0], (TOKENS, D_IN), 0.25, 4.0, ((0, 64), (1, 8)), (0, 1, 64, 4.0)),
        "queries": draw_queries(jax.random.fold_in(seeds[6], 71), 0),
        "key_values": draw_key_values(jax.random.fold_in(seeds[6], 71), 0),
        "attention_out": centred(seeds[3], (TOKENS, HEADS * HD), 1.0, 6.0, ((0, 64), (1, 8))),
        "output_grad": centred(seeds[4], (TOKENS, HEADS * HD), 4.0, 24.0, ((0, 64), (1, 8))),
        "document_start": draw_document_start(jax.random.fold_in(seeds[6], 71), 0),
    }


def reference(layer_input, queries, key_values, attention_out, output_grad, document_start):
    repeat = HEADS // KV_HEADS
    scaling = 1.0 / math.sqrt(HD)
    margin = REACH * TOK_DEV
    window = margin + TOK_DEV
    padded_pairs = jnp.concatenate([jnp.zeros((2, margin, KV_HEADS * HD), key_values.dtype), key_values], axis=1)
    offsets = jnp.arange(TOK_DEV, dtype=jnp.int32)
    window_offsets = jnp.arange(window, dtype=jnp.int32)
    highest = lax.Precision.HIGHEST

    def one_block(carry_grads, index):
        first_row = (index * TOK_DEV).astype(jnp.int32)
        query_heads = lax.dynamic_slice_in_dim(queries, first_row, TOK_DEV, 0).astype(jnp.float32).reshape(TOK_DEV, KV_HEADS, repeat, HD)
        grad_heads = lax.dynamic_slice_in_dim(output_grad, first_row, TOK_DEV, 0).astype(jnp.float32).reshape(TOK_DEV, KV_HEADS, repeat, HD)
        output_heads = lax.dynamic_slice_in_dim(attention_out, first_row, TOK_DEV, 0).astype(jnp.float32).reshape(TOK_DEV, KV_HEADS, repeat, HD)
        starts = lax.dynamic_slice_in_dim(document_start, first_row, TOK_DEV, 0)
        pair_block = lax.dynamic_slice_in_dim(padded_pairs, first_row, window, 1).astype(jnp.float32)
        key_heads = pair_block[0].reshape(window, KV_HEADS, HD)
        value_heads = pair_block[1].reshape(window, KV_HEADS, HD)
        query_pos = first_row + offsets
        key_pos = first_row - margin + window_offsets
        allowed = (key_pos[None, :] >= starts[:, None]) & (key_pos[None, :] <= query_pos[:, None])
        scores = jnp.einsum('igrd,jgd->grij', query_heads, key_heads, precision=highest) * scaling
        scores = jnp.where(allowed[None, None], scores, -jnp.inf)
        row_max = lax.optimization_barrier(jnp.max(scores, axis=3))
        log_total = row_max + jnp.log(lax.optimization_barrier(jnp.sum(jnp.exp(scores - row_max[..., None]), axis=3)))
        weights = jnp.exp(scores - log_total[..., None])
        weights_half = lax.optimization_barrier(weights.astype(jnp.bfloat16)).astype(jnp.float32)
        row_delta = lax.optimization_barrier(jnp.sum(grad_heads * output_heads, axis=3)).transpose(1, 2, 0)
        value_part = jnp.einsum('grij,igrd->jgd', weights_half, grad_heads, precision=highest)
        dot_grad = jnp.einsum('igrd,jgd->grij', grad_heads, value_heads, precision=highest)
        score_grad = (weights * (dot_grad - row_delta[..., None]) * scaling).astype(jnp.bfloat16)
        score_grad = lax.optimization_barrier(score_grad).astype(jnp.float32)
        query_part = jnp.einsum('grij,jgd->igrd', score_grad, key_heads, precision=highest).reshape(TOK_DEV, HEADS * HD)
        key_part = jnp.einsum('grij,igrd->jgd', score_grad, query_heads, precision=highest)
        update = jnp.stack((key_part.reshape(window, KV_HEADS * HD), value_part.reshape(window, KV_HEADS * HD)))
        previous = lax.dynamic_slice_in_dim(carry_grads, first_row, window, 1)
        carry_grads = lax.dynamic_update_slice_in_dim(carry_grads, previous + update, first_row, 1)
        return (carry_grads, query_part)
    initial = jnp.zeros((2, margin + TOKENS, KV_HEADS * HD), jnp.float32)
    indices = jnp.arange(TOKENS // TOK_DEV, dtype=jnp.int32)
    summed, query_blocks = lax.scan(one_block, initial, indices)
    query_grad = query_blocks.reshape(TOKENS, HEADS * HD).astype(jnp.bfloat16)
    key_value_grad = summed[:, margin:, :].astype(jnp.bfloat16)
    query_weight_grad = jnp.dot(layer_input.T, query_grad, preferred_element_type=jnp.float32)
    return (query_grad, key_value_grad, query_weight_grad)
```

```python
import math

import jax
import jax.numpy as jnp
from jax import lax
from jax.experimental import pallas as pl
from jax.experimental.pallas import tpu as pltpu
from jax.sharding import Mesh, PartitionSpec as P

HD = 128
REACH = 2
SEQ = ("x", "z", "c")
XS, ZS, CS, YS = 4, 8, 2, 8


def moved(shard, axis, size, by, wrap):
    pairs = [(i, (i + by) % size) for i in range(size) if wrap or 0 <= i + by < size]
    return lax.ppermute(shard, axis, pairs)


def dot(a, b, ca, cb):
    return lax.dot_general(a, b, (((ca,), (cb,)), ((), ())), preferred_element_type=jnp.float32)


def attention_backward(queries, attention_out, output_grad, document_start, near, one, two):
    rows = queries.shape[0]
    heads = queries.shape[1] // HD
    span = rows * (REACH + 1)
    scaling = 1.0 / math.sqrt(HD)

    def body(starts, q_ref, o_ref, g_ref, near_ref, one_ref, two_ref, dq_ref, own_ref, d1_ref, d2_ref, acc):
        head = pl.program_id(0)
        first = lax.axis_index(SEQ) * rows - REACH * rows
        q = q_ref[...]
        g = g_ref[...]
        keys = jnp.concatenate([two_ref[0], one_ref[0], near_ref[0]], axis=0)
        values = jnp.concatenate([two_ref[1], one_ref[1], near_ref[1]], axis=0)
        key_at = lax.broadcasted_iota(jnp.int32, (span, rows), 0)
        query_at = lax.broadcasted_iota(jnp.int32, (1, rows), 1) + REACH * rows
        allowed = (key_at >= starts[...] - first) & (key_at <= query_at)
        scores = jnp.where(allowed, dot(keys, q, 1, 1) * scaling, -jnp.inf)
        row_max = jnp.max(scores, axis=0, keepdims=True)
        powers = jnp.exp(scores - row_max)
        weights = powers * (1.0 / jnp.sum(powers, axis=0, keepdims=True))
        product = g.astype(jnp.float32) * o_ref[...].astype(jnp.float32)
        delta = jnp.sum(product.T, axis=0, keepdims=True)
        dot_grad = dot(values, g, 1, 1)
        score_grad = (weights * (dot_grad - delta) * scaling).astype(jnp.bfloat16)
        value_part = dot(weights.astype(jnp.bfloat16), g, 1, 0)
        key_part = dot(score_grad, q, 1, 0)
        dq_ref[...] = dot(keys, score_grad, 0, 0).T.astype(jnp.bfloat16)

        @pl.when(head == 0)
        def _():
            acc[0] = key_part
            acc[1] = value_part

        @pl.when(head > 0)
        def _():
            acc[0] += key_part
            acc[1] += value_part

        @pl.when(head == heads - 1)
        def _():
            d2_ref[...] = acc[:, :rows].astype(jnp.bfloat16)
            d1_ref[...] = acc[:, rows : 2 * rows].astype(jnp.bfloat16)
            own_ref[...] = acc[:, 2 * rows :]

    by_head = pl.BlockSpec((rows, HD), lambda h: (0, h))
    pair = pl.BlockSpec((2, rows, HD), lambda h: (0, 0, 0))
    return pl.pallas_call(
        body,
        grid=(heads,),
        in_specs=[pl.BlockSpec((1, rows), lambda h: (0, 0)), by_head, by_head, by_head, pair, pair, pair],
        out_specs=[by_head, pair, pair, pair],
        out_shape=[
            jax.ShapeDtypeStruct(queries.shape, jnp.bfloat16),
            jax.ShapeDtypeStruct((2, rows, HD), jnp.float32),
            jax.ShapeDtypeStruct((2, rows, HD), jnp.bfloat16),
            jax.ShapeDtypeStruct((2, rows, HD), jnp.bfloat16),
        ],
        scratch_shapes=[pltpu.VMEM((2, span, HD), jnp.float32)],
        name="attention_backward",
    )(document_start.reshape(1, rows), queries, attention_out, output_grad, near, one, two)


def weight_parts(pieces, query_grad):
    tokens, width = pieces[0].shape
    columns = query_grad.shape[1]
    owners = width // 64

    def body(*refs):
        shards, dq_ref, keep_ref, send_ref = refs[:YS], refs[YS], refs[YS + 1], refs[YS + 2]
        y = lax.axis_index("y")
        first_core = lax.axis_index("c") == 0
        dq = dq_ref[...]
        for d in range(YS):
            term = dot(shards[d][...], dq, 0, 0).astype(jnp.bfloat16).reshape(owners, 2, 32, columns)
            at = lax.rem(y + YS - d, YS) * owners
            keep_ref[pl.ds(at, owners)] = jnp.where(first_core, term[:, 0], term[:, 1])
            send_ref[pl.ds(at, owners)] = jnp.where(first_core, term[:, 1], term[:, 0])

    shape = jax.ShapeDtypeStruct((YS * owners, 32, columns), jnp.bfloat16)
    return pl.pallas_call(body, out_shape=[shape, shape], name="weight_parts")(*pieces, query_grad)


def shards(layer_input, queries, key_values, attention_out, output_grad, document_start):
    pieces = [layer_input] + [None] * (YS - 1)
    forward = backward = layer_input
    one = two = None
    for step in range(1, YS // 2 + 1):
        forward = moved(forward, "y", YS, 1, True)
        pieces[step] = forward
        if step < YS // 2:
            backward = moved(backward, "y", YS, -1, True)
            pieces[YS - step] = backward
        if step == 1:
            one = moved(key_values, SEQ, XS * ZS * CS, 1, False)
            two = moved(key_values, SEQ, XS * ZS * CS, 2, False)
    query_grad, own, part_one, part_two = attention_backward(
        queries, attention_out, output_grad, document_start, key_values, one, two
    )
    keep, send = weight_parts(pieces, query_grad)
    summed = keep + lax.ppermute(send, "c", [(0, 1), (1, 0)])
    arrived = lax.all_to_all(summed, ("x", "z"), split_axis=0, concat_axis=0, tiled=True)
    back_one = moved(part_one, SEQ, XS * ZS * CS, -1, False)
    back_two = moved(part_two, SEQ, XS * ZS * CS, -2, False)
    pair_total = own + back_one.astype(jnp.float32) + back_two.astype(jnp.float32)
    weight_grad = arrived.astype(jnp.float32).sum(axis=0)
    return query_grad, pair_total.astype(jnp.bfloat16), weight_grad


def solution(mesh):
    split = Mesh(mesh.devices.reshape(XS, ZS, CS, YS), SEQ + ("y",))
    placed = (
        P(SEQ, "y"),
        P(SEQ, "y"),
        P(None, SEQ, "y"),
        P(SEQ, "y"),
        P(SEQ, "y"),
        P(SEQ),
    )
    return jax.shard_map(
        shards,
        mesh=split,
        in_specs=placed,
        out_specs=(P(SEQ, "y"), P(None, SEQ, "y"), P(SEQ, "y")),
        check_vma=False,
    )
```

```python
import math

import jax
import jax.numpy as jnp
from jax import lax
from jax.experimental import pallas as pl
from jax.experimental.pallas import tpu as pltpu
from jax.sharding import Mesh, PartitionSpec as P


HD = 128
REACH = 2
SEQ = ("x", "z", "c")
XS, ZS, CS, YS = 4, 8, 2, 8


def moved(shard, axis, size, by, wrap):
    pairs = [(i, (i + by) % size) for i in range(size) if wrap or 0 <= i + by < size]
    return lax.ppermute(shard, axis, pairs)


def dot(a, b, ca, cb):
    return lax.dot_general(a, b, (((ca,), (cb,)), ((), ())), preferred_element_type=jnp.float32)


def attention_backward(queries, attention_out, output_grad, document_start, near, one, two):
    rows = queries.shape[0]
    heads = queries.shape[1] // HD
    span = rows * (REACH + 1)
    scaling = 1.0 / math.sqrt(HD)

    def body(starts, q_ref, o_ref, g_ref, near_ref, one_ref, two_ref, dq_ref, own_ref, d1_ref, d2_ref, acc):
        head = pl.program_id(0)
        first = lax.axis_index(SEQ) * rows - REACH * rows
        q = q_ref[...]
        g = g_ref[...]
        keys = jnp.concatenate([two_ref[0], one_ref[0], near_ref[0]], axis=0)
        values = jnp.concatenate([two_ref[1], one_ref[1], near_ref[1]], axis=0)
        key_at = lax.broadcasted_iota(jnp.int32, (span, rows), 0)
        query_at = lax.broadcasted_iota(jnp.int32, (1, rows), 1) + REACH * rows
        allowed = (key_at >= starts[...] - first) & (key_at <= query_at)
        scores = jnp.where(allowed, dot(keys, q, 1, 1) * scaling, -jnp.inf)
        row_max = jnp.max(scores, axis=0, keepdims=True)
        powers = jnp.exp(scores - row_max)
        weights = powers * (1.0 / jnp.sum(powers, axis=0, keepdims=True))
        product = g.astype(jnp.float32) * o_ref[...].astype(jnp.float32)
        delta = jnp.sum(product.T, axis=0, keepdims=True)
        dot_grad = dot(values, g, 1, 1)
        score_grad = (weights * (dot_grad - delta) * scaling).astype(jnp.bfloat16)
        value_part = dot(weights.astype(jnp.bfloat16), g, 1, 0)
        key_part = dot(score_grad, q, 1, 0)
        dq_ref[...] = dot(keys, score_grad, 0, 0).T.astype(jnp.bfloat16)

        @pl.when(head == 0)
        def _():
            acc[0] = key_part
            acc[1] = value_part

        @pl.when(head > 0)
        def _():
            acc[0] += key_part
            acc[1] += value_part

        @pl.when(head == heads - 1)
        def _():
            d2_ref[...] = acc[:, :rows].astype(jnp.bfloat16)
            d1_ref[...] = acc[:, rows : 2 * rows].astype(jnp.bfloat16)
            own_ref[...] = acc[:, 2 * rows :]

    by_head = pl.BlockSpec((rows, HD), lambda h: (0, h))
    pair = pl.BlockSpec((2, rows, HD), lambda h: (0, 0, 0))
    return pl.pallas_call(
        body,
        grid=(heads,),
        in_specs=[pl.BlockSpec((1, rows), lambda h: (0, 0)), by_head, by_head, by_head, pair, pair, pair],
        out_specs=[by_head, pair, pair, pair],
        out_shape=[
            jax.ShapeDtypeStruct(queries.shape, jnp.bfloat16),
            jax.ShapeDtypeStruct((2, rows, HD), jnp.float32),
            jax.ShapeDtypeStruct((2, rows, HD), jnp.bfloat16),
            jax.ShapeDtypeStruct((2, rows, HD), jnp.bfloat16),
        ],
        scratch_shapes=[pltpu.VMEM((2, span, HD), jnp.float32)],
        name="attention_backward",
    )(document_start.reshape(1, rows), queries, attention_out, output_grad, near, one, two)


def weight_term(features, mine, other):
    blocks, _, width, tokens = features.shape
    columns = mine.shape[2]

    def body(f_ref, mine_ref, other_ref, out_ref):
        x = lax.axis_index("x")
        c = lax.axis_index("c")
        even = lax.rem(x, 2) == 0
        beside = jnp.where(even, x + 1, x - 1)
        total = None
        for at, place in enumerate((x, beside, XS - 1 - x, XS - 1 - beside)):
            for source, rows in ((CS * place + c, mine_ref), (CS * place + 1 - c, other_ref)):
                left = f_ref[:, pl.ds(source, 1)].reshape(blocks * width, tokens)
                term = dot(left, rows[at], 1, 0)
                total = term if total is None else total + term
        out_ref[...] = total.astype(jnp.bfloat16).reshape(blocks, width, columns)

    shape = jax.ShapeDtypeStruct((blocks, width, columns), jnp.bfloat16)
    return pl.pallas_call(body, out_shape=shape, name="weight_term")(features, mine, other)


A = [(x, x ^ 1) for x in range(XS)]
B = [(x, XS - 1 - x) for x in range(XS)]


def exchanged(shard, pairs):
    return lax.ppermute(shard, "x", pairs)


def sent_to_all(shard, axis, size):
    copies = jnp.broadcast_to(shard, (size, *shard.shape))
    return lax.all_to_all(copies, axis, split_axis=0, concat_axis=0, tiled=True)


def step(layer_input, queries, key_values, attention_out, output_grad, document_start):
    rows = layer_input.shape[0]
    one = moved(key_values, SEQ, XS * ZS * CS, 1, False)
    two = moved(key_values, SEQ, XS * ZS * CS, 2, False)
    width = layer_input.shape[1] // (XS * CS)
    features = layer_input.T.reshape(XS * CS, width, rows)
    features = lax.all_to_all(features, ("x", "c"), split_axis=0, concat_axis=0, tiled=True)
    features = sent_to_all(features.reshape(XS * CS * width, rows), "y", YS)
    features = features.reshape(YS, XS * CS, width, rows)
    query_grad, own, part_one, part_two = attention_backward(
        queries, attention_out, output_grad, document_start, key_values, one, two
    )
    back_one = moved(part_one, SEQ, XS * ZS * CS, -1, False)
    back_two = moved(part_two, SEQ, XS * ZS * CS, -2, False)
    pair_total = own + back_one.astype(jnp.float32) + back_two.astype(jnp.float32)
    pair_total = pair_total.astype(jnp.bfloat16)
    low, high = query_grad[: rows // 2], query_grad[rows // 2 :]
    low_a, high_b = exchanged(low, A), exchanged(high, B)
    low_b = exchanged(jnp.concatenate([low, low_a]), B)
    high_a = exchanged(jnp.concatenate([high, high_b]), A)
    low_b, low_ab = jnp.split(low_b, 2)
    high_a, high_ab = jnp.split(high_a, 2)
    mine = jnp.concatenate([query_grad, low_a, high_a, low_b, high_b, low_ab, high_ab])
    mine = mine.reshape(XS, rows, query_grad.shape[1])
    other = lax.ppermute(mine, "c", [(0, 1), (1, 0)])
    term = weight_term(features, mine, other)
    arrived = lax.all_to_all(term, "z", split_axis=0, concat_axis=0, tiled=True)
    summed = arrived.astype(jnp.float32).sum(axis=0)
    half = ZS // 2
    owners = [(x * ZS + z, (z // 2) * ZS + half * (z % 2) + x) for x in range(XS) for z in range(ZS)]
    return query_grad, pair_total, lax.ppermute(summed, ("x", "z"), owners)


def solution(mesh):
    split = Mesh(mesh.devices.reshape(XS, ZS, CS, YS), SEQ + ("y",))
    placed = (
        P(SEQ, "y"),
        P(SEQ, "y"),
        P(None, SEQ, "y"),
        P(SEQ, "y"),
        P(SEQ, "y"),
        P(SEQ),
    )
    return jax.shard_map(
        step,
        mesh=split,
        in_specs=placed,
        out_specs=(P(SEQ, "y"), P(None, SEQ, "y"), P(SEQ, "y")),
        check_vma=False,
    )
```

```python
import math

import jax
import jax.numpy as jnp
from jax import lax
from jax.experimental import pallas as pl
from jax.experimental.pallas import tpu as pltpu
from jax.sharding import Mesh, PartitionSpec as P


HD = 128
REACH = 2
SEQ = ("x", "zh", "zl", "c")
XS, ZH, ZL, CS, YS = 4, 4, 2, 2, 8
SHARDS = XS * ZH * ZL * CS


def moved(shard, axis, size, by, wrap):
    pairs = [(i, (i + by) % size) for i in range(size) if wrap or 0 <= i + by < size]
    return lax.ppermute(shard, axis, pairs)


def dot(a, b, ca, cb):
    return lax.dot_general(a, b, (((ca,), (cb,)), ((), ())), preferred_element_type=jnp.float32)


def attention_backward(queries, attention_out, output_grad, document_start, near, one, two):
    rows = queries.shape[0]
    heads = queries.shape[1] // HD
    span = rows * (REACH + 1)
    scaling = 1.0 / math.sqrt(HD)

    def body(starts, q_ref, o_ref, g_ref, near_ref, one_ref, two_ref, dq_ref, own_ref, d1_ref, d2_ref, acc):
        head = pl.program_id(0)
        first = lax.axis_index(SEQ) * rows - REACH * rows
        q = q_ref[...]
        g = g_ref[...]
        keys = jnp.concatenate([two_ref[0], one_ref[0], near_ref[0]], axis=0)
        values = jnp.concatenate([two_ref[1], one_ref[1], near_ref[1]], axis=0)
        key_at = lax.broadcasted_iota(jnp.int32, (span, rows), 0)
        query_at = lax.broadcasted_iota(jnp.int32, (1, rows), 1) + REACH * rows
        allowed = (key_at >= starts[...] - first) & (key_at <= query_at)
        scores = jnp.where(allowed, dot(keys, q, 1, 1) * scaling, -jnp.inf)
        row_max = jnp.max(scores, axis=0, keepdims=True)
        powers = jnp.exp(scores - row_max)
        weights = powers * (1.0 / jnp.sum(powers, axis=0, keepdims=True))
        product = g.astype(jnp.float32) * o_ref[...].astype(jnp.float32)
        delta = jnp.sum(product.T, axis=0, keepdims=True)
        dot_grad = dot(values, g, 1, 1)
        score_grad = (weights * (dot_grad - delta) * scaling).astype(jnp.bfloat16)
        value_part = dot(weights.astype(jnp.bfloat16), g, 1, 0)
        key_part = dot(score_grad, q, 1, 0)
        dq_ref[...] = dot(keys, score_grad, 0, 0).T.astype(jnp.bfloat16)

        @pl.when(head == 0)
        def _():
            acc[0] = key_part
            acc[1] = value_part

        @pl.when(head > 0)
        def _():
            acc[0] += key_part
            acc[1] += value_part

        @pl.when(head == heads - 1)
        def _():
            d2_ref[...] = acc[:, :rows].astype(jnp.bfloat16)
            d1_ref[...] = acc[:, rows : 2 * rows].astype(jnp.bfloat16)
            own_ref[...] = acc[:, 2 * rows :]

    by_head = pl.BlockSpec((rows, HD), lambda h: (0, h))
    pair = pl.BlockSpec((2, rows, HD), lambda h: (0, 0, 0))
    return pl.pallas_call(
        body,
        grid=(heads,),
        in_specs=[pl.BlockSpec((1, rows), lambda h: (0, 0)), by_head, by_head, by_head, pair, pair, pair],
        out_specs=[by_head, pair, pair, pair],
        out_shape=[
            jax.ShapeDtypeStruct(queries.shape, jnp.bfloat16),
            jax.ShapeDtypeStruct((2, rows, HD), jnp.float32),
            jax.ShapeDtypeStruct((2, rows, HD), jnp.bfloat16),
            jax.ShapeDtypeStruct((2, rows, HD), jnp.bfloat16),
        ],
        scratch_shapes=[pltpu.VMEM((2, span, HD), jnp.float32)],
        name="attention_backward",
    )(document_start.reshape(1, rows), queries, attention_out, output_grad, near, one, two)


def weight_term(features, gathered):
    blocks, sources, width, tokens = features.shape
    columns = gathered[0].shape[1]

    def body(f_ref, *refs):
        rows, out_ref = refs[:-1], refs[-1]
        own = CS * lax.axis_index("zl") + lax.axis_index("c")
        swapped = CS * lax.axis_index("zl") + 1 - lax.axis_index("c")
        total = None
        for source, row in zip((own, swapped, sources - 1 - swapped, sources - 1 - own), rows):
            left = f_ref[:, pl.ds(source, 1)].reshape(blocks * width, tokens)
            term = dot(left, row[...], 1, 0)
            total = term if total is None else total + term
        out_ref[...] = total.astype(jnp.bfloat16).reshape(out_ref.shape)

    shape = jax.ShapeDtypeStruct((blocks * width // 32, 32, columns), jnp.bfloat16)
    return pl.pallas_call(body, out_shape=shape, name="weight_term")(features, *gathered)


def step(layer_input, queries, key_values, attention_out, output_grad, document_start):
    rows, features_here = layer_input.shape
    one = moved(key_values, SEQ, SHARDS, 1, False)
    two = moved(key_values, SEQ, SHARDS, 2, False)
    parts = layer_input.T.reshape(2, ZL * CS, features_here // (2 * ZL * CS), rows).swapaxes(0, 1)
    parts = parts.reshape(ZL * CS, features_here // (ZL * CS), rows)
    copies = jnp.broadcast_to(parts, (YS, *parts.shape)).reshape(YS * ZL * CS, *parts.shape[1:])
    features = lax.all_to_all(copies, ("y", "zl", "c"), split_axis=0, concat_axis=0, tiled=True)
    features = features.reshape(YS, *parts.shape)
    query_grad, own, part_one, part_two = attention_backward(
        queries, attention_out, output_grad, document_start, key_values, one, two
    )
    swap = [(0, 1), (1, 0)]
    beyond = lax.ppermute(query_grad, "zl", swap)
    beside = lax.ppermute(query_grad, "c", swap)
    across = lax.ppermute(beyond, "c", swap)
    back_one = moved(part_one, SEQ, SHARDS, -1, False)
    back_two = moved(part_two, SEQ, SHARDS, -2, False)
    pair_total = own + back_one.astype(jnp.float32) + back_two.astype(jnp.float32)
    pair_total = pair_total.astype(jnp.bfloat16)
    term = weight_term(features, (query_grad, beside, beyond, across))
    arrived = lax.all_to_all(term, ("x", "zh"), split_axis=0, concat_axis=0, tiled=True)
    return query_grad, pair_total, arrived.astype(jnp.float32).sum(axis=0)


def solution(mesh):
    split = Mesh(mesh.devices.reshape(XS, ZH, ZL, CS, YS), SEQ + ("y",))
    placed = (
        P(SEQ, "y"),
        P(SEQ, "y"),
        P(None, SEQ, "y"),
        P(SEQ, "y"),
        P(SEQ, "y"),
        P(SEQ),
    )
    return jax.shard_map(
        step,
        mesh=split,
        in_specs=placed,
        out_specs=(P(SEQ, "y"), P(None, SEQ, "y"), P(SEQ, "y")),
        check_vma=False,
    )
```

```python
import math

import jax
import jax.numpy as jnp
from jax import lax
from jax.experimental import pallas as pl
from jax.experimental.pallas import tpu as pltpu
from jax.sharding import Mesh, PartitionSpec as P


HD = 128
REACH = 2
SEQ = ("x", "zh", "zl", "c")
XS, ZH, ZL, CS, YS = 4, 4, 2, 2, 8
SHARDS = XS * ZH * ZL * CS


def moved(shard, axis, size, by, wrap):
    pairs = [(i, (i + by) % size) for i in range(size) if wrap or 0 <= i + by < size]
    return lax.ppermute(shard, axis, pairs)


def dot(a, b, ca, cb):
    return lax.dot_general(a, b, (((ca,), (cb,)), ((), ())), preferred_element_type=jnp.float32)


def in_vmem(array):
    return pltpu.with_memory_space_constraint(array, pltpu.VMEM)


def attention_backward(queries, attention_out, output_grad, document_start, near, one, two):
    rows = queries.shape[0]
    heads = queries.shape[1] // HD
    span = rows * (REACH + 1)
    scaling = 1.0 / math.sqrt(HD)

    def body(starts, q_ref, o_ref, g_ref, near_ref, one_ref, two_ref, dq_ref, own_ref, d1_ref, d2_ref, acc):
        head = pl.program_id(0)
        first = lax.axis_index(SEQ) * rows - REACH * rows
        q = q_ref[...]
        g = g_ref[...]
        keys = jnp.concatenate([two_ref[0], one_ref[0], near_ref[0]], axis=0)
        values = jnp.concatenate([two_ref[1], one_ref[1], near_ref[1]], axis=0)
        key_at = lax.broadcasted_iota(jnp.int32, (span, rows), 0)
        query_at = lax.broadcasted_iota(jnp.int32, (1, rows), 1) + REACH * rows
        allowed = (key_at >= starts[...] - first) & (key_at <= query_at)
        scores = jnp.where(allowed, dot(keys, q, 1, 1) * scaling, -jnp.inf)
        row_max = jnp.max(scores, axis=0, keepdims=True)
        powers = jnp.exp(scores - row_max)
        weights = powers * (1.0 / jnp.sum(powers, axis=0, keepdims=True))
        product = g.astype(jnp.float32) * o_ref[...].astype(jnp.float32)
        delta = jnp.sum(product.T, axis=0, keepdims=True)
        dot_grad = dot(values, g, 1, 1)
        score_grad = (weights * (dot_grad - delta) * scaling).astype(jnp.bfloat16)
        value_part = dot(weights.astype(jnp.bfloat16), g, 1, 0)
        key_part = dot(score_grad, q, 1, 0)
        dq_ref[...] = dot(keys, score_grad, 0, 0).T.astype(jnp.bfloat16)

        @pl.when(head == 0)
        def _():
            acc[0] = key_part
            acc[1] = value_part

        @pl.when(head > 0)
        def _():
            acc[0] += key_part
            acc[1] += value_part

        @pl.when(head == heads - 1)
        def _():
            d2_ref[...] = acc[:, :rows].astype(jnp.bfloat16)
            d1_ref[...] = acc[:, rows : 2 * rows].astype(jnp.bfloat16)
            own_ref[...] = acc[:, 2 * rows :]

    by_head = pl.BlockSpec((rows, HD), lambda h: (0, h))
    pair = pl.BlockSpec((2, rows, HD), lambda h: (0, 0, 0))
    whole = pl.BlockSpec(memory_space=pltpu.VMEM)
    return pl.pallas_call(
        body,
        grid=(heads,),
        in_specs=[pl.BlockSpec((1, rows), lambda h: (0, 0)), by_head, by_head, by_head, whole, whole, whole],
        out_specs=[by_head, pair, pair, pair],
        out_shape=[
            jax.ShapeDtypeStruct(queries.shape, jnp.bfloat16),
            jax.ShapeDtypeStruct((2, rows, HD), jnp.float32),
            jax.ShapeDtypeStruct((2, rows, HD), jnp.bfloat16),
            jax.ShapeDtypeStruct((2, rows, HD), jnp.bfloat16),
        ],
        scratch_shapes=[pltpu.VMEM((2, span, HD), jnp.float32)],
        name="attention_backward",
    )(document_start.reshape(1, rows), queries, attention_out, output_grad, *map(in_vmem, (near, one, two)))


def feature_copies(layer_input):
    rows, width = layer_input.shape
    owners = ZL * CS
    piece = width // (2 * owners)

    def body(x_ref, out_ref):
        turned = x_ref[...].T.reshape(2, owners, piece, rows)
        for owner in range(owners):
            for half in range(2):
                for y in range(YS):
                    out_ref[y * owners + owner, pl.ds(half * piece, piece)] = turned[half, owner]

    shape = jax.ShapeDtypeStruct((YS * owners, 2 * piece, rows), layer_input.dtype)
    return pl.pallas_call(body, out_shape=shape, name="feature_copies")(layer_input)


def weight_term(features, gathered):
    blocks, sources, width, tokens = features.shape
    columns = gathered[0].shape[1]

    def body(f_ref, *refs):
        rows, out_ref = refs[:-1], refs[-1]
        own = CS * lax.axis_index("zl") + lax.axis_index("c")
        swapped = CS * lax.axis_index("zl") + 1 - lax.axis_index("c")
        total = None
        for source, row in zip((own, swapped, sources - 1 - swapped, sources - 1 - own), rows):
            left = f_ref[:, pl.ds(source, 1)].reshape(blocks * width, tokens)
            term = dot(left, row[...], 1, 0)
            total = term if total is None else total + term
        out_ref[...] = total.astype(jnp.bfloat16).reshape(out_ref.shape)

    shape = jax.ShapeDtypeStruct((blocks * width // 32, 32, columns), jnp.bfloat16)
    whole = pl.BlockSpec(memory_space=pltpu.VMEM)
    specs = [whole] * (1 + len(gathered))
    return pl.pallas_call(body, in_specs=specs, out_shape=shape, name="weight_term")(*map(in_vmem, (features, *gathered)))


def step(layer_input, queries, key_values, attention_out, output_grad, document_start):
    one = moved(key_values, SEQ, SHARDS, 1, False)
    two = moved(key_values, SEQ, SHARDS, 2, False)
    copies = feature_copies(layer_input)
    features = lax.all_to_all(copies, ("y", "zl", "c"), split_axis=0, concat_axis=0, tiled=True)
    features = features.reshape(YS, ZL * CS, *copies.shape[1:])
    query_grad, own, part_one, part_two = attention_backward(
        queries, attention_out, output_grad, document_start, key_values, one, two
    )
    swap = [(0, 1), (1, 0)]
    beyond = lax.ppermute(query_grad, "zl", swap)
    beside = lax.ppermute(query_grad, "c", swap)
    across = lax.ppermute(beyond, "c", swap)
    back_one = moved(part_one, SEQ, SHARDS, -1, False)
    back_two = moved(part_two, SEQ, SHARDS, -2, False)
    pair_total = own + back_one.astype(jnp.float32) + back_two.astype(jnp.float32)
    pair_total = pair_total.astype(jnp.bfloat16)
    term = weight_term(features, (query_grad, beside, beyond, across))
    arrived = lax.all_to_all(term, ("x", "zh"), split_axis=0, concat_axis=0, tiled=True)
    return query_grad, pair_total, arrived.astype(jnp.float32).sum(axis=0)


def solution(mesh):
    split = Mesh(mesh.devices.reshape(XS, ZH, ZL, CS, YS), SEQ + ("y",))
    placed = (
        P(SEQ, "y"),
        P(SEQ, "y"),
        P(None, SEQ, "y"),
        P(SEQ, "y"),
        P(SEQ, "y"),
        P(SEQ),
    )
    return jax.shard_map(
        step,
        mesh=split,
        in_specs=placed,
        out_specs=(P(SEQ, "y"), P(None, SEQ, "y"), P(SEQ, "y")),
        check_vma=False,
    )
```

```python
import math

import jax
import jax.numpy as jnp
from jax import lax
from jax.experimental import pallas as pl
from jax.experimental.pallas import tpu as pltpu
from jax.sharding import Mesh, PartitionSpec as P


HD = 128
REACH = 2
SEQ = ("x", "zh", "zl", "c")
XS, ZH, ZL, CS, YS = 4, 4, 2, 2, 8
SHARDS = XS * ZH * ZL * CS


def moved(shard, axis, size, by, wrap):
    pairs = [(i, (i + by) % size) for i in range(size) if wrap or 0 <= i + by < size]
    return lax.ppermute(shard, axis, pairs)


def dot(a, b, ca, cb):
    return lax.dot_general(a, b, (((ca,), (cb,)), ((), ())), preferred_element_type=jnp.float32)


def in_vmem(array):
    return pltpu.with_memory_space_constraint(array, pltpu.VMEM)


def attention_backward(queries, attention_out, output_grad, document_start, near, one, two):
    rows = queries.shape[0]
    heads = queries.shape[1] // HD
    span = rows * (REACH + 1)
    scaling = 1.0 / math.sqrt(HD)

    def body(starts, q_ref, o_ref, g_ref, near_ref, one_ref, two_ref, dq_ref, own_ref, d1_ref, d2_ref, acc):
        head = pl.program_id(0)
        first = lax.axis_index(SEQ) * rows - REACH * rows
        q = q_ref[...]
        g = g_ref[...]
        keys = jnp.concatenate([two_ref[0], one_ref[0], near_ref[0]], axis=0)
        values = jnp.concatenate([two_ref[1], one_ref[1], near_ref[1]], axis=0)
        key_at = lax.broadcasted_iota(jnp.int32, (span, rows), 0)
        query_at = lax.broadcasted_iota(jnp.int32, (1, rows), 1) + REACH * rows
        allowed = (key_at >= starts[...] - first) & (key_at <= query_at)
        scores = jnp.where(allowed, dot(keys, q, 1, 1) * scaling, -jnp.inf)
        row_max = jnp.max(scores, axis=0, keepdims=True)
        powers = jnp.exp(scores - row_max)
        weights = powers * (1.0 / jnp.sum(powers, axis=0, keepdims=True))
        product = g.astype(jnp.float32) * o_ref[...].astype(jnp.float32)
        delta = jnp.sum(product.T, axis=0, keepdims=True)
        dot_grad = dot(values, g, 1, 1)
        score_grad = (weights * (dot_grad - delta) * scaling).astype(jnp.bfloat16)
        value_part = dot(weights.astype(jnp.bfloat16), g, 1, 0)
        key_part = dot(score_grad, q, 1, 0)
        dq_ref[...] = dot(keys, score_grad, 0, 0).T.astype(jnp.bfloat16)

        @pl.when(head == 0)
        def _():
            acc[0] = key_part
            acc[1] = value_part

        @pl.when(head > 0)
        def _():
            acc[0] += key_part
            acc[1] += value_part

        @pl.when(head == heads - 1)
        def _():
            d2_ref[...] = acc[:, :rows].astype(jnp.bfloat16)
            d1_ref[...] = acc[:, rows : 2 * rows].astype(jnp.bfloat16)
            own_ref[...] = acc[:, 2 * rows :]

    by_head = pl.BlockSpec((rows, HD), lambda h: (0, h))
    pair = pl.BlockSpec((2, rows, HD), lambda h: (0, 0, 0))
    whole = pl.BlockSpec(memory_space=pltpu.VMEM)
    return pl.pallas_call(
        body,
        grid=(heads,),
        in_specs=[pl.BlockSpec((1, rows), lambda h: (0, 0)), by_head, by_head, by_head, whole, whole, whole],
        out_specs=[by_head, pair, pair, pair],
        out_shape=[
            jax.ShapeDtypeStruct(queries.shape, jnp.bfloat16),
            jax.ShapeDtypeStruct((2, rows, HD), jnp.float32),
            jax.ShapeDtypeStruct((2, rows, HD), jnp.bfloat16),
            jax.ShapeDtypeStruct((2, rows, HD), jnp.bfloat16),
        ],
        scratch_shapes=[pltpu.VMEM((2, span, HD), jnp.float32)],
        name="attention_backward",
    )(document_start.reshape(1, rows), queries, attention_out, output_grad, *map(in_vmem, (near, one, two)))


def feature_copies(layer_input):
    rows, width = layer_input.shape
    owners = ZL * CS
    piece = width // (2 * owners)

    def body(x_ref, out_ref):
        turned = x_ref[...].T.reshape(2, owners, piece, rows)
        for owner in range(owners):
            for half in range(2):
                for y in range(YS):
                    out_ref[y * owners + owner, pl.ds(half * piece, piece)] = turned[half, owner]

    shape = jax.ShapeDtypeStruct((YS * owners, 2 * piece, rows), layer_input.dtype)
    return pl.pallas_call(body, out_shape=shape, name="feature_copies")(layer_input)


def weight_term(features, own, gathered):
    blocks, sources, width, tokens = features.shape
    columns = own.shape[1]

    def body(f_ref, own_ref, beside_ref, beyond_ref, across_ref, out_ref, own_here, arrived):
        fetch = pltpu.make_async_copy(own_ref, own_here, arrived)
        fetch.start()
        here = CS * lax.axis_index("zl") + lax.axis_index("c")
        partner = CS * lax.axis_index("zl") + 1 - lax.axis_index("c")

        def term(source, rows):
            left = f_ref[:, pl.ds(source, 1)].reshape(blocks * width, tokens)
            return dot(left, rows[...], 1, 0)

        total = term(partner, beside_ref) + term(sources - 1 - partner, beyond_ref)
        total += term(sources - 1 - here, across_ref)
        fetch.wait()
        total += term(here, own_here)
        out_ref[...] = total.astype(jnp.bfloat16).reshape(out_ref.shape)

    whole = pl.BlockSpec(memory_space=pltpu.VMEM)
    return pl.pallas_call(
        body,
        in_specs=[whole, pl.BlockSpec(memory_space=pl.ANY), whole, whole, whole],
        out_shape=jax.ShapeDtypeStruct((blocks * width // 32, 32, columns), jnp.bfloat16),
        scratch_shapes=[pltpu.VMEM(own.shape, own.dtype), pltpu.SemaphoreType.DMA(())],
        name="weight_term",
    )(in_vmem(features), own, *map(in_vmem, gathered))


def step(layer_input, queries, key_values, attention_out, output_grad, document_start):
    one = moved(key_values, SEQ, SHARDS, 1, False)
    two = moved(key_values, SEQ, SHARDS, 2, False)
    copies = feature_copies(layer_input)
    features = lax.all_to_all(copies, ("y", "zl", "c"), split_axis=0, concat_axis=0, tiled=True)
    features = features.reshape(YS, ZL * CS, *copies.shape[1:])
    query_grad, own, part_one, part_two = attention_backward(
        queries, attention_out, output_grad, document_start, key_values, one, two
    )
    swap = [(0, 1), (1, 0)]
    beyond = lax.ppermute(query_grad, "zl", swap)
    beside = lax.ppermute(query_grad, "c", swap)
    across = lax.ppermute(beyond, "c", swap)
    back_one = moved(part_one, SEQ, SHARDS, -1, False)
    back_two = moved(part_two, SEQ, SHARDS, -2, False)
    pair_total = own + back_one.astype(jnp.float32) + back_two.astype(jnp.float32)
    pair_total = pair_total.astype(jnp.bfloat16)
    term = weight_term(features, query_grad, (beside, beyond, across))
    arrived = lax.all_to_all(term, "x", split_axis=0, concat_axis=0, tiled=True)
    summed = arrived.reshape(XS, ZH, *arrived.shape[1:]).astype(jnp.float32).sum(axis=0).astype(jnp.bfloat16)
    arrived = lax.all_to_all(summed, "zh", split_axis=0, concat_axis=0, tiled=True)
    return query_grad, pair_total, arrived.astype(jnp.float32).sum(axis=0)


def solution(mesh):
    split = Mesh(mesh.devices.reshape(XS, ZH, ZL, CS, YS), SEQ + ("y",))
    placed = (
        P(SEQ, "y"),
        P(SEQ, "y"),
        P(None, SEQ, "y"),
        P(SEQ, "y"),
        P(SEQ, "y"),
        P(SEQ),
    )
    return jax.shard_map(
        step,
        mesh=split,
        in_specs=placed,
        out_specs=(P(SEQ, "y"), P(None, SEQ, "y"), P(SEQ, "y")),
        check_vma=False,
    )
```

```python
import math

import jax
import jax.numpy as jnp
from jax import lax
from jax.experimental import pallas as pl
from jax.experimental.pallas import tpu as pltpu
from jax.sharding import Mesh, PartitionSpec as P


HD = 128
REACH = 2
SEQ = ("x", "z", "c")
XS, ZS, CS, YS = 4, 8, 2, 8
SHARDS = XS * ZS * CS


def moved(shard, axis, size, by, wrap):
    pairs = [(i, (i + by) % size) for i in range(size) if wrap or 0 <= i + by < size]
    return lax.ppermute(shard, axis, pairs)


def dot(a, b, ca, cb):
    return lax.dot_general(a, b, (((ca,), (cb,)), ((), ())), preferred_element_type=jnp.float32)


def in_vmem(array):
    return pltpu.with_memory_space_constraint(array, pltpu.VMEM)


def attention_backward(queries, attention_out, output_grad, document_start, near, one, two):
    rows = queries.shape[0]
    heads = queries.shape[1] // HD
    span = rows * (REACH + 1)
    scaling = 1.0 / math.sqrt(HD)

    def body(starts, q_ref, o_ref, g_ref, near_ref, one_ref, two_ref, dq_ref, own_ref, d1_ref, d2_ref, acc):
        head = pl.program_id(0)
        first = lax.axis_index(SEQ) * rows - REACH * rows
        q = q_ref[...]
        g = g_ref[...]
        keys = jnp.concatenate([two_ref[0], one_ref[0], near_ref[0]], axis=0)
        values = jnp.concatenate([two_ref[1], one_ref[1], near_ref[1]], axis=0)
        key_at = lax.broadcasted_iota(jnp.int32, (span, rows), 0)
        query_at = lax.broadcasted_iota(jnp.int32, (1, rows), 1) + REACH * rows
        allowed = (key_at >= starts[...] - first) & (key_at <= query_at)
        scores = jnp.where(allowed, dot(keys, q, 1, 1) * scaling, -jnp.inf)
        row_max = jnp.max(scores, axis=0, keepdims=True)
        powers = jnp.exp(scores - row_max)
        weights = powers * (1.0 / jnp.sum(powers, axis=0, keepdims=True))
        product = g.astype(jnp.float32) * o_ref[...].astype(jnp.float32)
        delta = jnp.sum(product.T, axis=0, keepdims=True)
        dot_grad = dot(values, g, 1, 1)
        score_grad = (weights * (dot_grad - delta) * scaling).astype(jnp.bfloat16)
        value_part = dot(weights.astype(jnp.bfloat16), g, 1, 0)
        key_part = dot(score_grad, q, 1, 0)
        dq_ref[...] = dot(keys, score_grad, 0, 0).T.astype(jnp.bfloat16)

        @pl.when(head == 0)
        def _():
            acc[0] = key_part
            acc[1] = value_part

        @pl.when(head > 0)
        def _():
            acc[0] += key_part
            acc[1] += value_part

        @pl.when(head == heads - 1)
        def _():
            d2_ref[...] = acc[:, :rows].astype(jnp.bfloat16)
            d1_ref[...] = acc[:, rows : 2 * rows].astype(jnp.bfloat16)
            own_ref[...] = acc[:, 2 * rows :]

    by_head = pl.BlockSpec((rows, HD), lambda h: (0, h))
    pair = pl.BlockSpec((2, rows, HD), lambda h: (0, 0, 0))
    whole = pl.BlockSpec(memory_space=pltpu.VMEM)
    return pl.pallas_call(
        body,
        grid=(heads,),
        in_specs=[pl.BlockSpec((1, rows), lambda h: (0, 0)), by_head, by_head, by_head, whole, whole, whole],
        out_specs=[by_head, pair, pair, pair],
        out_shape=[
            jax.ShapeDtypeStruct(queries.shape, jnp.bfloat16),
            jax.ShapeDtypeStruct((2, rows, HD), jnp.float32),
            jax.ShapeDtypeStruct((2, rows, HD), jnp.bfloat16),
            jax.ShapeDtypeStruct((2, rows, HD), jnp.bfloat16),
        ],
        scratch_shapes=[pltpu.VMEM((2, span, HD), jnp.float32)],
        name="attention_backward",
    )(document_start.reshape(1, rows), queries, attention_out, output_grad, *map(in_vmem, (near, one, two)))


def feature_copies(layer_input):
    rows, width = layer_input.shape
    pieces = width // (CS * 32)

    def body(x_ref, out_ref):
        turned = x_ref[...].T.reshape(pieces, CS, 32, rows)
        for core in range(CS):
            mine = turned[:, core].reshape(pieces * 32, rows)
            for y in range(YS):
                out_ref[y * CS + core] = mine

    shape = jax.ShapeDtypeStruct((YS * CS, pieces * 32, rows), layer_input.dtype)
    return pl.pallas_call(body, out_shape=shape, name="feature_copies")(layer_input)


def weight_term(features, own, beside):
    blocks, _, width, tokens = features.shape
    columns = own.shape[1]

    def body(f_ref, own_ref, beside_ref, out_ref, own_here, arrived):
        fetch = pltpu.make_async_copy(own_ref, own_here, arrived)
        fetch.start()
        core = lax.axis_index("c")

        def term(source, rows):
            left = f_ref[:, pl.ds(source, 1)].reshape(blocks * width, tokens)
            return dot(left, rows[...], 1, 0)

        total = term(1 - core, beside_ref)
        fetch.wait()
        total += term(core, own_here)
        out_ref[...] = total.astype(jnp.bfloat16).reshape(out_ref.shape)

    whole = pl.BlockSpec(memory_space=pltpu.VMEM)
    return pl.pallas_call(
        body,
        in_specs=[whole, pl.BlockSpec(memory_space=pl.ANY), whole],
        out_shape=jax.ShapeDtypeStruct((blocks * width // 32, 32, columns), jnp.bfloat16),
        scratch_shapes=[pltpu.VMEM(own.shape, own.dtype), pltpu.SemaphoreType.DMA(())],
        name="weight_term",
    )(in_vmem(features), own, in_vmem(beside))


def step(layer_input, queries, key_values, attention_out, output_grad, document_start):
    one = moved(key_values, SEQ, SHARDS, 1, False)
    two = moved(key_values, SEQ, SHARDS, 2, False)
    copies = feature_copies(layer_input)
    features = lax.all_to_all(copies, ("y", "c"), split_axis=0, concat_axis=0, tiled=True)
    features = features.reshape(YS, CS, *copies.shape[1:])
    query_grad, own, part_one, part_two = attention_backward(
        queries, attention_out, output_grad, document_start, key_values, one, two
    )
    beside = lax.ppermute(query_grad, "c", [(0, 1), (1, 0)])
    back_one = moved(part_one, SEQ, SHARDS, -1, False)
    back_two = moved(part_two, SEQ, SHARDS, -2, False)
    pair_total = own + back_one.astype(jnp.float32) + back_two.astype(jnp.float32)
    pair_total = pair_total.astype(jnp.bfloat16)
    term = weight_term(features, query_grad, beside)
    arrived = lax.all_to_all(term, "x", split_axis=0, concat_axis=0, tiled=True)
    summed = arrived.reshape(XS, ZS, *arrived.shape[1:]).astype(jnp.float32).sum(axis=0).astype(jnp.bfloat16)
    arrived = lax.all_to_all(summed, "z", split_axis=0, concat_axis=0, tiled=True)
    return query_grad, pair_total, arrived.astype(jnp.float32).sum(axis=0)


def solution(mesh):
    split = Mesh(mesh.devices.reshape(XS, ZS, CS, YS), SEQ + ("y",))
    placed = (
        P(SEQ, "y"),
        P(SEQ, "y"),
        P(None, SEQ, "y"),
        P(SEQ, "y"),
        P(SEQ, "y"),
        P(SEQ),
    )
    return jax.shard_map(
        step,
        mesh=split,
        in_specs=placed,
        out_specs=(P(SEQ, "y"), P(None, SEQ, "y"), P(SEQ, "y")),
        check_vma=False,
    )
```

```python
import math

import jax
import jax.numpy as jnp
from jax import lax
from jax.experimental import pallas as pl
from jax.experimental.pallas import tpu as pltpu
from jax.sharding import Mesh, PartitionSpec as P


HD = 128
REACH = 2
SEQ = ("x", "zh", "zl", "c")
XS, ZH, ZL, CS, YS = 4, 4, 2, 2, 8
SHARDS = XS * ZH * ZL * CS


def moved(shard, axis, size, by, wrap):
    pairs = [(i, (i + by) % size) for i in range(size) if wrap or 0 <= i + by < size]
    return lax.ppermute(shard, axis, pairs)


def dot(a, b, ca, cb):
    return lax.dot_general(a, b, (((ca,), (cb,)), ((), ())), preferred_element_type=jnp.float32)


def in_vmem(array):
    return pltpu.with_memory_space_constraint(array, pltpu.VMEM)


def attention_backward(queries, attention_out, output_grad, document_start, near, one, two):
    rows = queries.shape[0]
    heads = queries.shape[1] // HD
    span = rows * (REACH + 1)
    scaling = 1.0 / math.sqrt(HD)

    def body(starts, q_ref, o_ref, g_ref, near_ref, one_ref, two_ref, dq_ref, own_ref, d1_ref, d2_ref, acc):
        head = pl.program_id(0)
        first = lax.axis_index(SEQ) * rows - REACH * rows
        q = q_ref[...]
        g = g_ref[...]
        keys = jnp.concatenate([two_ref[0], one_ref[0], near_ref[0]], axis=0)
        values = jnp.concatenate([two_ref[1], one_ref[1], near_ref[1]], axis=0)
        key_at = lax.broadcasted_iota(jnp.int32, (span, rows), 0)
        query_at = lax.broadcasted_iota(jnp.int32, (1, rows), 1) + REACH * rows
        allowed = (key_at >= starts[...] - first) & (key_at <= query_at)
        scores = jnp.where(allowed, dot(keys, q, 1, 1) * scaling, -jnp.inf)
        row_max = jnp.max(scores, axis=0, keepdims=True)
        powers = jnp.exp(scores - row_max)
        weights = powers * (1.0 / jnp.sum(powers, axis=0, keepdims=True))
        product = g.astype(jnp.float32) * o_ref[...].astype(jnp.float32)
        delta = jnp.sum(product.T, axis=0, keepdims=True)
        dot_grad = dot(values, g, 1, 1)
        score_grad = (weights * (dot_grad - delta) * scaling).astype(jnp.bfloat16)
        value_part = dot(weights.astype(jnp.bfloat16), g, 1, 0)
        key_part = dot(score_grad, q, 1, 0)
        dq_ref[...] = dot(keys, score_grad, 0, 0).T.astype(jnp.bfloat16)

        @pl.when(head == 0)
        def _():
            acc[0] = key_part
            acc[1] = value_part

        @pl.when(head > 0)
        def _():
            acc[0] += key_part
            acc[1] += value_part

        @pl.when(head == heads - 1)
        def _():
            d2_ref[...] = acc[:, :rows].astype(jnp.bfloat16)
            d1_ref[...] = acc[:, rows : 2 * rows].astype(jnp.bfloat16)
            own_ref[...] = acc[:, 2 * rows :]

    by_head = pl.BlockSpec((rows, HD), lambda h: (0, h))
    pair = pl.BlockSpec((2, rows, HD), lambda h: (0, 0, 0))
    whole = pl.BlockSpec(memory_space=pltpu.VMEM)
    return pl.pallas_call(
        body,
        grid=(heads,),
        in_specs=[pl.BlockSpec((1, rows), lambda h: (0, 0)), by_head, by_head, by_head, whole, whole, whole],
        out_specs=[by_head, pair, pair, pair],
        out_shape=[
            jax.ShapeDtypeStruct(queries.shape, jnp.bfloat16),
            jax.ShapeDtypeStruct((2, rows, HD), jnp.float32),
            jax.ShapeDtypeStruct((2, rows, HD), jnp.bfloat16),
            jax.ShapeDtypeStruct((2, rows, HD), jnp.bfloat16),
        ],
        scratch_shapes=[pltpu.VMEM((2, span, HD), jnp.float32)],
        name="attention_backward",
    )(document_start.reshape(1, rows), queries, attention_out, output_grad, *map(in_vmem, (near, one, two)))


def feature_halves(layer_input):
    rows, width = layer_input.shape
    upper = width // (32 * ZL * CS)

    def body(x_ref, keep_ref, send_ref):
        turned = x_ref[...].T.reshape(upper, ZL, CS, 32, rows)
        even = lax.axis_index("zl") == 0
        keep = jnp.where(even, turned[:, 0], turned[:, 1])
        send = jnp.where(even, turned[:, 1], turned[:, 0])
        for core in range(CS):
            keep_ref[core] = keep[:, core].reshape(upper * 32, rows)
            send_ref[core] = send[:, core].reshape(upper * 32, rows)

    shape = jax.ShapeDtypeStruct((CS, upper * 32, rows), layer_input.dtype)
    return pl.pallas_call(body, out_shape=[shape, shape], name="feature_halves")(layer_input)


def feature_copies(kept, got):
    def body(kept_ref, got_ref, out_ref):
        for y in range(YS):
            for core in range(CS):
                out_ref[y * CS + core, 0] = kept_ref[core]
                out_ref[y * CS + core, 1] = got_ref[core]

    shape = jax.ShapeDtypeStruct((YS * CS, ZL, *kept.shape[1:]), kept.dtype)
    return pl.pallas_call(body, out_shape=shape, name="feature_copies")(kept, in_vmem(got))


def weight_term(features, own, gathered):
    blocks, _, width, tokens = features.shape
    columns = own.shape[1]

    def body(f_ref, own_ref, beside_ref, beyond_ref, across_ref, out_ref, own_here, arrived):
        fetch = pltpu.make_async_copy(own_ref, own_here, arrived)
        fetch.start()
        here = ZL * lax.axis_index("c")
        partner = ZL - here

        def term(source, rows):
            left = f_ref[:, pl.ds(source, 1)].reshape(blocks * width, tokens)
            return dot(left, rows[...], 1, 0)

        total = term(partner, beside_ref) + term(here + 1, beyond_ref)
        total += term(partner + 1, across_ref)
        fetch.wait()
        total += term(here, own_here)
        out_ref[...] = total.astype(jnp.bfloat16).reshape(out_ref.shape)

    whole = pl.BlockSpec(memory_space=pltpu.VMEM)
    return pl.pallas_call(
        body,
        in_specs=[whole, pl.BlockSpec(memory_space=pl.ANY), whole, whole, whole],
        out_shape=jax.ShapeDtypeStruct((blocks * width // 32, 32, columns), jnp.bfloat16),
        scratch_shapes=[pltpu.VMEM(own.shape, own.dtype), pltpu.SemaphoreType.DMA(())],
        name="weight_term",
    )(in_vmem(features), own, *map(in_vmem, gathered))


def step(layer_input, queries, key_values, attention_out, output_grad, document_start):
    one = moved(key_values, SEQ, SHARDS, 1, False)
    two = moved(key_values, SEQ, SHARDS, 2, False)
    swap = [(0, 1), (1, 0)]
    kept, sent = feature_halves(layer_input)
    got = lax.ppermute(sent, "zl", swap)
    copies = feature_copies(kept, got)
    features = lax.all_to_all(copies, ("y", "c"), split_axis=0, concat_axis=0, tiled=True)
    features = features.reshape(YS, CS * ZL, *copies.shape[2:])
    query_grad, own, part_one, part_two = attention_backward(
        queries, attention_out, output_grad, document_start, key_values, one, two
    )
    beyond = lax.ppermute(query_grad, "zl", swap)
    beside = lax.ppermute(query_grad, "c", swap)
    across = lax.ppermute(beyond, "c", swap)
    back_one = moved(part_one, SEQ, SHARDS, -1, False)
    back_two = moved(part_two, SEQ, SHARDS, -2, False)
    pair_total = own + back_one.astype(jnp.float32) + back_two.astype(jnp.float32)
    pair_total = pair_total.astype(jnp.bfloat16)
    term = weight_term(features, query_grad, (beside, beyond, across))
    arrived = lax.all_to_all(term, ("x", "zh"), split_axis=0, concat_axis=0, tiled=True)
    return query_grad, pair_total, arrived.astype(jnp.float32).sum(axis=0)


def solution(mesh):
    split = Mesh(mesh.devices.reshape(XS, ZH, ZL, CS, YS), SEQ + ("y",))
    placed = (
        P(SEQ, "y"),
        P(SEQ, "y"),
        P(None, SEQ, "y"),
        P(SEQ, "y"),
        P(SEQ, "y"),
        P(SEQ),
    )
    return jax.shard_map(
        step,
        mesh=split,
        in_specs=placed,
        out_specs=(P(SEQ, "y"), P(None, SEQ, "y"), P(SEQ, "y")),
        check_vma=False,
    )
```

```python
import functools
import math

import jax
import jax.numpy as jnp
from jax import lax
from jax.experimental import pallas as pl
from jax.experimental.pallas import tpu as pltpu
from jax.sharding import Mesh, PartitionSpec as P


HD = 128
REACH = 2
BLOCK = 256
SEQ = ("x", "zh", "zl", "c")
XS, ZH, ZL, CS, YS = 4, 4, 2, 2, 8
SHARDS = XS * ZH * ZL * CS


def moved(shard, axis, size, by, wrap):
    pairs = [(i, (i + by) % size) for i in range(size) if wrap or 0 <= i + by < size]
    return lax.ppermute(shard, axis, pairs)


def dot(a, b, ca, cb):
    return lax.dot_general(a, b, (((ca,), (cb,)), ((), ())), preferred_element_type=jnp.float32)


def in_vmem(array):
    return pltpu.with_memory_space_constraint(array, pltpu.VMEM)


def attention_backward(queries, attention_out, output_grad, document_start, near, one, two):
    rows = queries.shape[0]
    heads = queries.shape[1] // HD
    span = rows * (REACH + 1)
    scaling = 1.0 / math.sqrt(HD)

    def body(starts, q_ref, o_ref, g_ref, near_ref, one_ref, two_ref, dq_ref, own_ref, d1_ref, d2_ref, acc):
        head = pl.program_id(0)
        first = lax.axis_index(SEQ) * rows - REACH * rows
        q = q_ref[...]
        g = g_ref[...]
        starting = starts[...] - first
        query_at = lax.broadcasted_iota(jnp.int32, (1, rows), 1) + REACH * rows
        blocks = [(ref, at) for ref in (two_ref, one_ref, near_ref) for at in range(0, rows, BLOCK)]
        scores = []
        for n, (ref, at) in enumerate(blocks):
            key_at = lax.broadcasted_iota(jnp.int32, (BLOCK, rows), 0) + n * BLOCK
            allowed = (key_at >= starting) & (key_at <= query_at)
            scores.append(jnp.where(allowed, dot(ref[0, pl.ds(at, BLOCK)], q, 1, 1), -jnp.inf))
        row_max = functools.reduce(jnp.maximum, [jnp.max(s, axis=0, keepdims=True) for s in scores])
        powers = [jnp.exp2((s - row_max) * (scaling * math.log2(math.e))) for s in scores]
        inverse = 1.0 / sum(jnp.sum(p, axis=0, keepdims=True) for p in powers)
        product = g.astype(jnp.float32) * o_ref[...].astype(jnp.float32)
        delta = jnp.sum(product.T, axis=0, keepdims=True)

        @pl.when(head == 0)
        def _():
            acc[...] = jnp.zeros_like(acc)

        query_part = None
        for n, (ref, at) in enumerate(blocks):
            weights = powers[n] * inverse
            dot_grad = dot(ref[1, pl.ds(at, BLOCK)], g, 1, 1)
            score_grad = (weights * (dot_grad - delta) * scaling).astype(jnp.bfloat16)
            acc[1, pl.ds(n * BLOCK, BLOCK)] += dot(weights.astype(jnp.bfloat16), g, 1, 0)
            acc[0, pl.ds(n * BLOCK, BLOCK)] += dot(score_grad, q, 1, 0)
            part = dot(ref[0, pl.ds(at, BLOCK)], score_grad, 0, 0)
            query_part = part if query_part is None else query_part + part
        dq_ref[...] = query_part.T.astype(jnp.bfloat16)

        @pl.when(head == heads - 1)
        def _():
            d2_ref[...] = acc[:, :rows].astype(jnp.bfloat16)
            d1_ref[...] = acc[:, rows : 2 * rows].astype(jnp.bfloat16)
            own_ref[...] = acc[:, 2 * rows :]

    by_head = pl.BlockSpec((rows, HD), lambda h: (0, h))
    pair = pl.BlockSpec((2, rows, HD), lambda h: (0, 0, 0))
    whole = pl.BlockSpec(memory_space=pltpu.VMEM)
    return pl.pallas_call(
        body,
        grid=(heads,),
        in_specs=[pl.BlockSpec((1, rows), lambda h: (0, 0)), by_head, by_head, by_head, whole, whole, whole],
        out_specs=[by_head, pair, pair, pair],
        out_shape=[
            jax.ShapeDtypeStruct(queries.shape, jnp.bfloat16),
            jax.ShapeDtypeStruct((2, rows, HD), jnp.float32),
            jax.ShapeDtypeStruct((2, rows, HD), jnp.bfloat16),
            jax.ShapeDtypeStruct((2, rows, HD), jnp.bfloat16),
        ],
        scratch_shapes=[pltpu.VMEM((2, span, HD), jnp.float32)],
        name="attention_backward",
    )(document_start.reshape(1, rows), queries, attention_out, output_grad, *map(in_vmem, (near, one, two)))


def feature_copies(layer_input):
    rows, width = layer_input.shape
    owners = ZL * CS
    piece = width // (2 * owners)

    def body(x_ref, out_ref):
        turned = x_ref[...].T.reshape(2, owners, piece, rows)
        for owner in range(owners):
            for half in range(2):
                for y in range(YS):
                    out_ref[y * owners + owner, pl.ds(half * piece, piece)] = turned[half, owner]

    shape = jax.ShapeDtypeStruct((YS * owners, 2 * piece, rows), layer_input.dtype)
    return pl.pallas_call(body, out_shape=shape, name="feature_copies")(layer_input)


def weight_term(features, own, gathered):
    blocks, sources, width, tokens = features.shape
    columns = own.shape[1]

    def body(f_ref, own_ref, beside_ref, beyond_ref, across_ref, out_ref, own_here, arrived):
        fetch = pltpu.make_async_copy(own_ref, own_here, arrived)
        fetch.start()
        here = CS * lax.axis_index("zl") + lax.axis_index("c")
        partner = CS * lax.axis_index("zl") + 1 - lax.axis_index("c")

        def term(source, rows):
            left = f_ref[:, pl.ds(source, 1)].reshape(blocks * width, tokens)
            return dot(left, rows[...], 1, 0)

        total = term(partner, beside_ref) + term(sources - 1 - partner, beyond_ref)
        total += term(sources - 1 - here, across_ref)
        fetch.wait()
        total += term(here, own_here)
        out_ref[...] = total.astype(jnp.bfloat16).reshape(out_ref.shape)

    whole = pl.BlockSpec(memory_space=pltpu.VMEM)
    return pl.pallas_call(
        body,
        in_specs=[whole, pl.BlockSpec(memory_space=pl.ANY), whole, whole, whole],
        out_shape=jax.ShapeDtypeStruct((blocks * width // 32, 32, columns), jnp.bfloat16),
        scratch_shapes=[pltpu.VMEM(own.shape, own.dtype), pltpu.SemaphoreType.DMA(())],
        name="weight_term",
    )(in_vmem(features), own, *map(in_vmem, gathered))


def step(layer_input, queries, key_values, attention_out, output_grad, document_start):
    one = moved(key_values, SEQ, SHARDS, 1, False)
    two = moved(key_values, SEQ, SHARDS, 2, False)
    copies = feature_copies(layer_input)
    features = lax.all_to_all(copies, ("y", "zl", "c"), split_axis=0, concat_axis=0, tiled=True)
    features = features.reshape(YS, ZL * CS, *copies.shape[1:])
    query_grad, own, part_one, part_two = attention_backward(
        queries, attention_out, output_grad, document_start, key_values, one, two
    )
    swap = [(0, 1), (1, 0)]
    beyond = lax.ppermute(query_grad, "zl", swap)
    beside = lax.ppermute(query_grad, "c", swap)
    across = lax.ppermute(beyond, "c", swap)
    back_one = moved(part_one, SEQ, SHARDS, -1, False)
    back_two = moved(part_two, SEQ, SHARDS, -2, False)
    pair_total = own + back_one.astype(jnp.float32) + back_two.astype(jnp.float32)
    pair_total = pair_total.astype(jnp.bfloat16)
    term = weight_term(features, query_grad, (beside, beyond, across))
    arrived = lax.all_to_all(term, ("x", "zh"), split_axis=0, concat_axis=0, tiled=True)
    return query_grad, pair_total, arrived.astype(jnp.float32).sum(axis=0)


def solution(mesh):
    split = Mesh(mesh.devices.reshape(XS, ZH, ZL, CS, YS), SEQ + ("y",))
    placed = (
        P(SEQ, "y"),
        P(SEQ, "y"),
        P(None, SEQ, "y"),
        P(SEQ, "y"),
        P(SEQ, "y"),
        P(SEQ),
    )
    return jax.shard_map(
        step,
        mesh=split,
        in_specs=placed,
        out_specs=(P(SEQ, "y"), P(None, SEQ, "y"), P(SEQ, "y")),
        check_vma=False,
    )
```

```python
import functools
import math

import jax
import jax.numpy as jnp
from jax import lax
from jax.experimental import pallas as pl
from jax.experimental.pallas import tpu as pltpu
from jax.sharding import Mesh, PartitionSpec as P


HD = 128
REACH = 2
BLOCK = 256
SEQ = ("x", "zh", "zl", "c")
XS, ZH, ZL, CS, YS = 4, 4, 2, 2, 8
SHARDS = XS * ZH * ZL * CS


def moved(shard, axis, size, by, wrap):
    pairs = [(i, (i + by) % size) for i in range(size) if wrap or 0 <= i + by < size]
    return lax.ppermute(shard, axis, pairs)


def dot(a, b, ca, cb):
    return lax.dot_general(a, b, (((ca,), (cb,)), ((), ())), preferred_element_type=jnp.float32)


def in_vmem(array):
    return pltpu.with_memory_space_constraint(array, pltpu.VMEM)


def attention_backward(queries, attention_out, output_grad, document_start, near, one, two):
    rows = queries.shape[0]
    heads = queries.shape[1] // HD
    span = rows * (REACH + 1)
    scaling = 1.0 / math.sqrt(HD)

    def body(starts, q_ref, o_ref, g_ref, near_ref, one_ref, two_ref, dq_ref, own_ref, d1_ref, d2_ref, acc):
        head = pl.program_id(0)
        first = lax.axis_index(SEQ) * rows - REACH * rows
        q = q_ref[...]
        g = g_ref[...]
        starting = starts[...] - first
        query_at = lax.broadcasted_iota(jnp.int32, (1, rows), 1) + REACH * rows
        blocks = [(ref, at) for ref in (two_ref, one_ref, near_ref) for at in range(0, rows, BLOCK)]
        scores = []
        for n, (ref, at) in enumerate(blocks):
            key_at = lax.broadcasted_iota(jnp.int32, (BLOCK, rows), 0) + n * BLOCK
            allowed = (key_at >= starting) & (key_at <= query_at)
            scores.append(jnp.where(allowed, dot(ref[0, pl.ds(at, BLOCK)], q, 1, 1), -jnp.inf))
        row_max = functools.reduce(jnp.maximum, [jnp.max(s, axis=0, keepdims=True) for s in scores])
        powers = [jnp.exp2((s - row_max) * (scaling * math.log2(math.e))) for s in scores]
        inverse = 1.0 / sum(jnp.sum(p, axis=0, keepdims=True) for p in powers)
        product = g.astype(jnp.float32) * o_ref[...].astype(jnp.float32)
        delta = jnp.sum(product.T, axis=0, keepdims=True)

        @pl.when(head == 0)
        def _():
            acc[...] = jnp.zeros_like(acc)

        query_part = None
        for n, (ref, at) in enumerate(blocks):
            weights = powers[n] * inverse
            dot_grad = dot(ref[1, pl.ds(at, BLOCK)], g, 1, 1)
            score_grad = (weights * (dot_grad - delta) * scaling).astype(jnp.bfloat16)
            acc[1, pl.ds(n * BLOCK, BLOCK)] += dot(weights.astype(jnp.bfloat16), g, 1, 0)
            acc[0, pl.ds(n * BLOCK, BLOCK)] += dot(score_grad, q, 1, 0)
            part = dot(ref[0, pl.ds(at, BLOCK)], score_grad, 0, 0)
            query_part = part if query_part is None else query_part + part
        dq_ref[...] = query_part.T.astype(jnp.bfloat16)

        @pl.when(head == heads - 1)
        def _():
            d2_ref[...] = acc[:, :rows].astype(jnp.bfloat16)
            d1_ref[...] = acc[:, rows : 2 * rows].astype(jnp.bfloat16)
            own_ref[...] = acc[:, 2 * rows :]

    by_head = pl.BlockSpec((rows, HD), lambda h: (0, h))
    pair = pl.BlockSpec((2, rows, HD), lambda h: (0, 0, 0))
    whole = pl.BlockSpec(memory_space=pltpu.VMEM)
    return pl.pallas_call(
        body,
        grid=(heads,),
        in_specs=[pl.BlockSpec((1, rows), lambda h: (0, 0)), by_head, by_head, by_head, whole, whole, whole],
        out_specs=[by_head, pair, pair, pair],
        out_shape=[
            jax.ShapeDtypeStruct(queries.shape, jnp.bfloat16),
            jax.ShapeDtypeStruct((2, rows, HD), jnp.float32),
            jax.ShapeDtypeStruct((2, rows, HD), jnp.bfloat16),
            jax.ShapeDtypeStruct((2, rows, HD), jnp.bfloat16),
        ],
        scratch_shapes=[pltpu.VMEM((2, span, HD), jnp.float32)],
        name="attention_backward",
    )(document_start.reshape(1, rows), queries, attention_out, output_grad, *map(in_vmem, (near, one, two)))


def feature_copies(layer_input):
    rows, width = layer_input.shape
    owners = ZL * CS
    piece = width // (2 * owners)

    def body(x_ref, out_ref):
        turned = x_ref[...].T.reshape(2, owners, piece, rows)
        for owner in range(owners):
            for half in range(2):
                for y in range(YS):
                    place = (owner % CS * ZL + owner // CS) * YS + y
                    out_ref[place, pl.ds(half * piece, piece)] = turned[half, owner]

    shape = jax.ShapeDtypeStruct((YS * owners, 2 * piece, rows), layer_input.dtype)
    return pl.pallas_call(body, out_shape=shape, name="feature_copies")(layer_input)


def weight_term(features, own, gathered):
    sources, blocks, width, tokens = features.shape
    columns = own.shape[1]

    def body(f_ref, own_ref, beside_ref, beyond_ref, across_ref, out_ref, own_here, arrived):
        fetch = pltpu.make_async_copy(own_ref, own_here, arrived)
        fetch.start()
        here = ZL * lax.axis_index("c") + lax.axis_index("zl")
        partner = ZL * (1 - lax.axis_index("c")) + lax.axis_index("zl")

        def term(source, rows):
            left = f_ref[pl.ds(source, 1)].reshape(blocks * width, tokens)
            return dot(left, rows[...], 1, 0)

        total = term(partner, beside_ref) + term(sources - 1 - partner, beyond_ref)
        total += term(sources - 1 - here, across_ref)
        fetch.wait()
        total += term(here, own_here)
        by_owner = total.astype(jnp.bfloat16).reshape(XS, ZH, *out_ref.shape[1:])
        for zh in range(ZH):
            for x in range(XS):
                out_ref[zh * XS + x] = by_owner[x, zh]

    whole = pl.BlockSpec(memory_space=pltpu.VMEM)
    return pl.pallas_call(
        body,
        in_specs=[whole, pl.BlockSpec(memory_space=pl.ANY), whole, whole, whole],
        out_shape=jax.ShapeDtypeStruct((blocks * width // 32, 32, columns), jnp.bfloat16),
        scratch_shapes=[pltpu.VMEM(own.shape, own.dtype), pltpu.SemaphoreType.DMA(())],
        name="weight_term",
    )(in_vmem(features), own, *map(in_vmem, gathered))


def step(layer_input, queries, key_values, attention_out, output_grad, document_start):
    one = moved(key_values, SEQ, SHARDS, 1, False)
    two = moved(key_values, SEQ, SHARDS, 2, False)
    copies = feature_copies(layer_input)
    features = lax.all_to_all(copies, ("c", "zl", "y"), split_axis=0, concat_axis=0, tiled=True)
    features = features.reshape(CS * ZL, YS, *copies.shape[1:])
    query_grad, own, part_one, part_two = attention_backward(
        queries, attention_out, output_grad, document_start, key_values, one, two
    )
    swap = [(0, 1), (1, 0)]
    beyond = lax.ppermute(query_grad, "zl", swap)
    beside = lax.ppermute(query_grad, "c", swap)
    across = lax.ppermute(beyond, "c", swap)
    back_one = moved(part_one, SEQ, SHARDS, -1, False)
    back_two = moved(part_two, SEQ, SHARDS, -2, False)
    pair_total = own + back_one.astype(jnp.float32) + back_two.astype(jnp.float32)
    pair_total = pair_total.astype(jnp.bfloat16)
    term = weight_term(features, query_grad, (beside, beyond, across))
    arrived = lax.all_to_all(term, ("zh", "x"), split_axis=0, concat_axis=0, tiled=True)
    return query_grad, pair_total, arrived.astype(jnp.float32).sum(axis=0)


def solution(mesh):
    split = Mesh(mesh.devices.reshape(XS, ZH, ZL, CS, YS), SEQ + ("y",))
    placed = (
        P(SEQ, "y"),
        P(SEQ, "y"),
        P(None, SEQ, "y"),
        P(SEQ, "y"),
        P(SEQ, "y"),
        P(SEQ),
    )
    return jax.shard_map(
        step,
        mesh=split,
        in_specs=placed,
        out_specs=(P(SEQ, "y"), P(None, SEQ, "y"), P(SEQ, "y")),
        check_vma=False,
    )
```
